128 devices in a mesh: dp: 16 (over z, x_lo, core), mp: 8 (over x_hi, y).
Axes of the slice: x: 4 (x_hi: 2, x_lo: 2; x = x_hi * 2 + x_lo), y: 4, z: 4, core: 2. Of those that a mesh axis runs over, the one named last changes fastest.
Arguments:
- master: float32 [8192, 5120], P('dp', 'mp'), may hold values from -60 to 60
- moment_first: float32 [8192, 5120], P('dp', 'mp'), may hold values from -0.06 to 0.06
- moment_second: float32 [8192, 5120], P('dp', 'mp'), may hold values from 1e-05 to 0.001
- gradients: float32 [8192, 5120], P('dp', 'mp'), may hold values from -0.2 to 0.2
- step_count: int32 [1], replicated, may hold values from 1 to 10
- tensor_rows: int32 [24], replicated, may hold values from 1 to 1280, 8192 in all
- decay_mask: int32 [24], replicated, may hold values 0 or 1
Outputs:
- new_master: float32 [8192, 5120], P('dp', 'mp')
- new_first: float32 [8192, 5120], P('dp', 'mp')
- new_second: float32 [8192, 5120], P('dp', 'mp')
- compute_weights: bfloat16 [8192, 5120], P(None, 'mp')
The draws below stay inside these ranges and needn't reach their ends.
Inputs may be any that keep to these rules, and one draw needn't show every extreme that they name: `tensor_rows`: the rows sum to 8192; the largest tensor has 1280 rows.
All inputs are finite; a program needn't handle non-finite values.
Results may differ from the reference program's by a relative error of at most 0.0004.
Values may be sent and summed in bfloat16 or wider, within the bound.
A program may use at most 128 MiB of HBM per device.

```python
import math
import jax
import jax.numpy as jnp
import numpy as np
from jax import lax

WIDE = 5120
TENSORS = 24
ROWS = 8192
MOST = 1280


def draw_master(key, part):
    keys = jax.random.split(key, 3)
    row_scale = jnp.exp(jax.random.uniform(keys[0], (ROWS, 1), jnp.float32, -1.2, 1.2))
    col_scale = jnp.exp(jax.random.uniform(keys[1], (1, WIDE), jnp.float32, -1.2, 1.2))
    ramp = 1.0 + 2.0 * jnp.arange(ROWS, dtype=jnp.float32)[:, None] / ROWS
    base = jax.random.normal(keys[2], (ROWS, WIDE), jnp.float32)
    values = 0.3 * base * row_scale * col_scale * ramp
    return jnp.clip(values, -60.0, 60.0).astype(jnp.float32)


def set_ends(entries, key, low, top_value):
    longest = entries.shape.index(max(entries.shape))
    spots = []
    for shift in (0, 1):
        where = [jax.random.randint(jax.random.fold_in(key, axis), (), 0, length) for axis, length in enumerate(entries.shape)]
        where[longest] = (where[longest] + shift) % entries.shape[longest]
        spots.append(tuple(where))
    return entries.at[spots[0]].set(low).at[spots[1]].set(top_value)


def block_levels(own_key, dims, shards, low, high):
    level = 1.0
    for axis_at, shards_of in shards:
        draws = jax.random.uniform(jax.random.fold_in(jax.random.fold_in(own_key, 6), axis_at), (shards_of,), jnp.float32, low / len(shards), high / len(shards))
        level = level * jnp.repeat(jnp.exp(draws), dims[axis_at] // shards_of).reshape((-1,) + (1,) * (len(dims) - 1 - axis_at))
    return level


def profile(count, total, limit, slope):
    loads = [(1 << 20) // math.isqrt(grade ** slope) + 1 for grade in range(2, count + 1)]
    rest, counts = total - limit - (count - 1), [1] * (count - 1)
    while rest > 0:
        movable = [i for i in range(count - 1) if counts[i] < limit]
        pool, budget = sum([loads[i] for i in movable]), rest
        for i in movable:
            more = min(limit - counts[i], max(1, budget * loads[i] // pool), rest)
            counts[i] = counts[i] + more
            rest = rest - more
    return np.array([limit] + counts)


def ragged_sizes(stream_key, amount, total, most, slope):
    if amount == 2:
        one = jax.random.randint(stream_key, (), max(1, total - most), min(most, total - 1) + 1)
        return jnp.stack([one, total - one])
    tallies = jnp.asarray(profile(amount, total, most, slope), jnp.int32)
    pairs = (amount - 1) // 2
    source_of, taker = tallies[1:1 + 2 * pairs:2], tallies[2:2 + 2 * pairs:2]
    room = jnp.minimum(source_of - 1, most - taker)
    shifted = jax.random.randint(jax.random.fold_in(stream_key, 1), (pairs,), 0, 1 << 20) % (room + 1)
    tallies = tallies.at[1:1 + 2 * pairs:2].set(source_of - shifted).at[2:2 + 2 * pairs:2].set(taker + shifted)
    return tallies[jax.random.permutation(jax.random.fold_in(stream_key, 2), amount)]


def bell_draw(key, dims, width, bound, cuts=(), held_as=jnp.bfloat16):
    gain = block_levels(key, dims, cuts, -0.22, 0.18) if cuts else 1.0
    values = jax.random.normal(key, dims, jnp.float32) * width * gain
    return jnp.minimum(jnp.maximum(values, -bound), bound).astype(held_as)


def setup_inputs(seed: int = 0) -> dict:
    arg_keys = jax.random.split(jax.random.key(seed), 8)
    master = draw_master(jax.random.fold_in(arg_keys[7], 71), 0)
    moment_first = bell_draw(arg_keys[1], (ROWS, WIDE), 0.01, 0.06, ((0, 16), (1, 8)), jnp.float32)
    moment_second = jnp.clip(jnp.exp(math.log(0.001) - 4.6051703 * jax.random.uniform(arg_keys[2], (ROWS, WIDE), jnp.float32) ** block_levels(arg_keys[2], (ROWS, WIDE), ((0, 16), (1, 8)), -0.2, 0.2)), 9.999999747378752e-06, 0.001)
    gradients = bell_draw(arg_keys[3], (ROWS, WIDE), 0.03, 0.2, ((0, 16), (1, 8)), jnp.float32)
    step_count = jax.random.randint(arg_keys[4], (1,), 1, 11).astype(jnp.int32)
    tensor_rows = ragged_sizes(arg_keys[5], TENSORS, ROWS, MOST, 1).astype(jnp.int32)
    decay_mask = set_ends((jax.random.randint(arg_keys[6], (TENSORS,), 0, 2) < 1).astype(jnp.int32), jax.random.fold_in(arg_keys[6], 1), 0, 1)
    return dict(master=master, moment_first=moment_first, moment_second=moment_second, gradients=gradients, step_count=step_count, tensor_rows=tensor_rows, decay_mask=decay_mask)


beta_first = 0.9
beta_second = 0.999
adam_epsilon = 1e-06
decay_rate = 0.3
learn_rate = 0.3
norm_epsilon = 1e-06

def reference(master, moment_first, moment_second, gradients, step_count, tensor_rows, decay_mask):
    steps = step_count[0].astype(jnp.float32)
    new_first = beta_first * moment_first + (1.0 - beta_first) * gradients
    new_second = beta_second * moment_second + (1.0 - beta_second) * gradients * gradients
    fix_first = 1.0 - jnp.power(jnp.float32(beta_first), steps)
    fix_second = 1.0 - jnp.power(jnp.float32(beta_second), steps)
    offsets = (jnp.cumsum(tensor_rows) - tensor_rows).astype(jnp.int32)
    row_ids = jnp.arange(ROWS, dtype=jnp.int32)
    segment = (lax.optimization_barrier(jnp.sum((row_ids[:, None] >= offsets[None, :]).astype(jnp.int32), axis=1)) - 1).astype(jnp.int32)
    mask_rows = decay_mask.astype(jnp.float32)[segment]
    update = new_first / fix_first / (jnp.sqrt(new_second / fix_second) + adam_epsilon)
    update = update + decay_rate * mask_rows[:, None] * master
    weight_sq = jax.ops.segment_sum(lax.optimization_barrier(jnp.sum(master * master, axis=1)), segment, num_segments=TENSORS)
    update_sq = jax.ops.segment_sum(lax.optimization_barrier(jnp.sum(update * update, axis=1)), segment, num_segments=TENSORS)
    ratio = jnp.sqrt(weight_sq) / (jnp.sqrt(update_sq) + norm_epsilon)
    new_master = master - learn_rate * ratio[segment][:, None] * update
    return (new_master, new_first, new_second, new_master.astype(jnp.bfloat16))
```

```python
import functools

import jax
import jax.numpy as jnp
from jax import lax
from jax.experimental import pallas as pl
from jax.experimental.pallas import tpu as pltpu
from jax.sharding import PartitionSpec as P

MESH = pl.DeviceIdType.MESH

beta_first = 0.9
beta_second = 0.999
adam_epsilon = 1e-06
decay_rate = 0.3
learn_rate = 0.3
norm_epsilon = 1e-06

TENSORS = 24
ROWS = 512
COLS = 640
DP = 16
MP = 8
REACH = 3
PEERS = (2 * REACH + 1) * MP

LOAD = 64
LOADS = ROWS // LOAD
CH = 32
CHUNKS = ROWS // CH
A = tuple(range(9))
B = tuple(range(9, 16))
UP = frozenset((0, 2, 4, 6, 8, 10, 12, 14))
UP_CROSSED = frozenset((1, 3, 5, 7))


def forwards(kind, k):
    if kind == "up1":
        return (("up", "z2"),) * (k in UP) + (("x", "x_up"),) * (k in B)
    if kind == "down1":
        return (("down", "z2"),) * (k not in UP) + (("x", "x_down"),) * (k in B)
    if kind == "z2":
        return (("x", "x_z2"),) * (k in B)
    if kind == "x0":
        return (("up", "x_up"), ("down", "x_down")) if k in A else ()
    if kind == "x_up" and k in A:
        return (("up", "x_z2"),) * (k in UP_CROSSED)
    if kind == "x_down" and k in A:
        return (("down", "x_z2"),) * (k not in UP_CROSSED)
    return ()


def own_order():
    order = []
    for i in range(len(A)):
        order.append((A[i], "x"))
        if i < len(B):
            order += [(B[i], "up"), (B[i], "down")]
    for i in range(len(A)):
        order += [(A[i], "up"), (A[i], "down")]
        if i < len(B):
            order.append((B[i], "x"))
    return order


def arrival_order():
    first = {"up": "up1", "down": "down1", "x": "x0"}
    free = {"up": 0.0, "down": 0.0, "x": 0.0}
    pending, order = [], []

    def send(link, kind, k, now):
        free[link] = max(free[link], now) + 0.88
        pending.append((free[link] + 2.0, len(pending) + len(order), kind, k))

    for k, link in own_order():
        send(link, first[link], k, 0.0)
    while pending:
        pending.sort()
        now, _, kind, k = pending.pop(0)
        order.append((kind, k))
        for link, there in forwards(kind, k):
            send(link, there, k, now)
    return order


ORDER = arrival_order()
SLOT = {item: n for n, item in enumerate(ORDER)}


def kernel(steps_ref, rows_hbm, decay_hbm, master_hbm, first_hbm, second_hbm, grad_hbm,
           master_out, first_out, second_out, weights,
           master, first, second, grad, update, decay_rows, part, parts, rows_ref, decay_ref, small_sem,
           load_sem, part_send, part_recv, up_send, down_send, x_send, core_send, recv_sem, core_recv):
    d, m = lax.axis_index("dp"), lax.axis_index("mp")
    z, x, c = d // 4, (d // 2) % 2, d % 2
    step = 1 + 2 * c
    z_up, z_down, z_far = (z + step) % 4, (z + 4 - step) % 4, (z + 2) % 4

    def device(zz, xx, cc):
        return (zz * 2 + xx) * 2 + cc

    target = {"up": device(z_up, x, c), "down": device(z_down, x, c), "x": device(z, 1 - x, c)}
    partner = device(z, x, 1 - c)
    send_sem = {"up": up_send, "down": down_send, "x": x_send}

    peers = []
    for reach in range(-REACH, REACH + 1):
        for hi in range(2):
            for y in range(4):
                if (reach, hi, y) != (0, 0, 0):
                    peers.append((-(2 * hi + min(y, 4 - y) + (abs(reach) + 1) // 2), reach, hi, y))
    peers = [
        ((d + DP + reach) % DP, (m // 4 + hi) % 2 * 4 + (m + y) % 4, reach)
        for _, reach, hi, y in sorted(peers)
    ]

    smalls = [
        pltpu.make_async_copy(src, dst, small_sem.at[n])
        for n, (src, dst) in enumerate(((rows_hbm, rows_ref), (decay_hbm, decay_ref)))
    ]
    for one in smalls:
        one.start()
    for n in range(LOADS):
        span = pl.ds(n * LOAD, LOAD)
        for a, (src, dst) in enumerate(
            ((master_hbm, master), (first_hbm, first), (second_hbm, second), (grad_hbm, grad))
        ):
            pltpu.make_async_copy(src.at[span], dst.at[span], load_sem.at[n, a]).start()

    barrier = pltpu.get_barrier_semaphore()
    for pd, pm, _ in peers:
        pl.semaphore_signal(barrier, inc=1, device_id=(pd, pm), device_id_type=MESH)
    for link in ("up", "down"):
        pl.semaphore_signal(barrier, inc=1, device_id=(target[link], m), device_id_type=MESH)

    lane = lax.broadcasted_iota(jnp.int32, (8, 128), 1)
    sub = lax.broadcasted_iota(jnp.int32, (8, 128), 0)
    for one in smalls:
        one.wait()
    start = jnp.zeros((8, 128), jnp.int32)
    end = jnp.zeros((8, 128), jnp.int32)
    decay = jnp.zeros((8, 128), jnp.float32)
    offset = jnp.int32(0)
    for t in range(TENSORS):
        here = lane % 32 == t
        after = offset + rows_ref[t]
        start = jnp.where(here, offset, start)
        end = jnp.where(here, after, end)
        decay = jnp.where(here, decay_ref[t].astype(jnp.float32) * decay_rate, decay)
        offset = after
    decay = jnp.where(lane < 32, decay, 0.0)

    steps = jnp.full((8, 128), steps_ref[0], jnp.int32)
    power_first = jnp.ones((8, 128), jnp.float32)
    power_second = jnp.ones((8, 128), jnp.float32)
    base_first, base_second = jnp.float32(beta_first), jnp.float32(beta_second)
    base_first = jnp.full((8, 128), base_first)
    base_second = jnp.full((8, 128), base_second)
    for _ in range(31):
        odd = steps % 2 == 1
        power_first = jnp.where(odd, power_first * base_first, power_first)
        power_second = jnp.where(odd, power_second * base_second, power_second)
        base_first, base_second, steps = base_first * base_first, base_second * base_second, steps // 2
    inv_first = (1.0 / (1.0 - power_first))[:, :1]
    inv_second = (1.0 / (1.0 - power_second))[:, :1]

    first_row = d * ROWS

    def member(row):
        ids = sub + (first_row + row)
        return (ids >= start) & (ids < end)

    def decay_step(n, carry):
        for g in range(8):
            row = n * 64 + g * 8
            value = jnp.sum(jnp.where(member(row), decay, 0.0), axis=1, keepdims=True)
            decay_rows[pl.ds(pl.multiple_of(row, 8), 8), :] = jnp.broadcast_to(value, (8, 128))
        return carry

    lax.fori_loop(0, ROWS // 64, decay_step, 0)

    def load_step(n, total):
        span = pl.ds(pl.multiple_of(n * LOAD, LOAD), LOAD)
        for a, (src, dst) in enumerate(
            ((master_hbm, master), (first_hbm, first), (second_hbm, second), (grad_hbm, grad))
        ):
            pltpu.make_async_copy(src.at[span], dst.at[span], load_sem.at[n, a]).wait()
        for g in range(LOAD // 8):
            row = n * LOAD + g * 8
            here = pl.ds(pl.multiple_of(row, 8), 8)
            w, gr = master[here, :], grad[here, :]
            new_first = beta_first * first[here, :] + (1.0 - beta_first) * gr
            new_second = beta_second * second[here, :] + (1.0 - beta_second) * gr * gr
            first_out[here, :] = new_first
            second_out[here, :] = new_second
            up = (new_first * inv_first) / (jnp.sqrt(new_second * inv_second) + adam_epsilon)
            up = up + decay_rows[here, :][:, :1] * w
            update[here, :] = up
            w_sum = jnp.sum(w * w, axis=1, keepdims=True)
            u_sum = jnp.sum(up * up, axis=1, keepdims=True)
            total = total + jnp.where(member(row), jnp.where(lane < 32, w_sum, u_sum), 0.0)
        return total

    total = lax.fori_loop(0, LOADS, load_step, jnp.zeros((8, 128), jnp.float32))
    total = jnp.sum(total, axis=0, keepdims=True)
    part[...] = total
    parts[REACH * MP + m] = total

    pl.semaphore_wait(barrier, len(peers) + 2)
    for pd, pm, reach in peers:
        pltpu.make_async_remote_copy(
            src_ref=part, dst_ref=parts.at[(reach + REACH) * MP + m], send_sem=part_send, recv_sem=part_recv,
            device_id=(pd, pm), device_id_type=MESH,
        ).start()
    others = parts.at[pl.ds(0, PEERS - 1)]
    pltpu.make_async_copy(others, others, part_recv).wait()

    sums = jnp.sum(parts[...], axis=0)
    sums = jnp.broadcast_to(sums, (8, 128))
    u_sq = pltpu.roll(sums, 96, 1)
    ratio = learn_rate * (jnp.sqrt(sums) / (jnp.sqrt(u_sq) + norm_epsilon))
    ratio = jnp.where(lane < TENSORS, ratio, 0.0)

    def chunk(dev, k):
        return weights.at[pl.ds(pl.multiple_of(dev * ROWS + k * CH, CH), CH)]

    def copy(link, kind, dev, k):
        return pltpu.make_async_remote_copy(
            src_ref=chunk(dev, k), dst_ref=chunk(dev, k), send_sem=send_sem[link], recv_sem=recv_sem.at[SLOT[kind, k]],
            device_id=(target[link], m), device_id_type=MESH,
        )

    def share(dev, k):
        pltpu.make_async_remote_copy(
            src_ref=chunk(dev, k), dst_ref=chunk(dev, k), send_sem=core_send, recv_sem=core_recv,
            device_id=(partner, m), device_id_type=MESH,
        ).start()

    def finish(k):
        for g in range(CH // 16):
            halves = []
            for h in range(2):
                row = k * CH + g * 16 + h * 8
                scale = jnp.sum(jnp.where(member(row), ratio, 0.0), axis=1, keepdims=True)
                halves.append(master[pl.ds(row, 8), :] - scale * update[pl.ds(row, 8), :])
            value = jnp.concatenate(halves, axis=0)
            row = k * CH + g * 16
            master_out[pl.ds(row, 16), :] = value
            weights[pl.ds(pl.multiple_of(d * ROWS + row, 16), 16), :] = value.astype(jnp.bfloat16)

    first_kind = {"up": "up1", "down": "down1", "x": "x0"}
    done = set()
    for k, link in own_order():
        if k not in done:
            finish(k)
        copy(link, first_kind[link], d, k).start()
        if k not in done:
            share(d, k)
            done.add(k)

    origin = {
        "up1": device(z_down, x, c), "down1": device(z_up, x, c), "z2": device(z_far, x, c),
        "x0": device(z, 1 - x, c), "x_up": device(z_down, 1 - x, c), "x_down": device(z_up, 1 - x, c),
        "x_z2": device(z_far, 1 - x, c),
    }
    sent = {"up": CHUNKS, "down": CHUNKS, "x": CHUNKS}
    for kind, k in ORDER:
        dev = origin[kind]
        copy("x", kind, dev, k).wait_recv()
        for link, there in forwards(kind, k):
            copy(link, there, dev, k).start()
            sent[link] += 1
        share(dev, k)

    def rows_of(count):
        return weights.at[pl.ds(0, count * CH)]

    pltpu.make_async_copy(rows_of(8 * CHUNKS), rows_of(8 * CHUNKS), core_recv).wait()
    pltpu.make_async_copy(rows_of(8 * CHUNKS), rows_of(8 * CHUNKS), core_send).wait()
    for link, count in sent.items():
        pltpu.make_async_copy(rows_of(count), rows_of(count), send_sem[link]).wait()
    pltpu.make_async_copy(others, others, part_send).wait()


def store_kernel(*refs):
    sources, sinks, sem = refs[:4], refs[4:8], refs[8]
    copies = []
    for n, (src, dst) in enumerate(zip(sources, sinks)):
        pieces = 8 if n == 3 else 1
        rows = src.shape[0] // pieces
        for i in range(pieces):
            span = pl.ds(i * rows, rows)
            copies.append(pltpu.make_async_copy(src.at[span], dst.at[span], sem.at[len(copies)]))
    for one in copies:
        one.start()
    for one in copies:
        one.wait()


def local(master, moment_first, moment_second, gradients, step_count, tensor_rows, decay_mask):
    hbm = pl.BlockSpec(memory_space=pltpu.MemorySpace.HBM)
    vmem = pl.BlockSpec(memory_space=pltpu.MemorySpace.VMEM)
    smem = pl.BlockSpec(memory_space=pltpu.MemorySpace.SMEM)
    f32 = jnp.float32
    block = (ROWS, COLS)
    results = pl.pallas_call(
        kernel,
        name="lamb_gather",
        out_shape=[pltpu.VMEM(block, f32)] * 3 + [pltpu.VMEM((DP * ROWS, COLS), jnp.bfloat16)],
        in_specs=[smem] + [hbm] * 6,
        out_specs=[vmem] * 4,
        scratch_shapes=[pltpu.VMEM(block, f32)] * 5 + [
            pltpu.VMEM((ROWS, 128), f32),
            pltpu.VMEM((1, 128), f32),
            pltpu.VMEM((PEERS, 1, 128), f32),
            pltpu.SMEM((TENSORS,), jnp.int32),
            pltpu.SMEM((TENSORS,), jnp.int32),
            pltpu.SemaphoreType.DMA((2,)),
            pltpu.SemaphoreType.DMA((LOADS, 4)),
        ] + [pltpu.SemaphoreType.DMA] * 6 + [
            pltpu.SemaphoreType.DMA((len(ORDER),)),
            pltpu.SemaphoreType.DMA,
        ],
        compiler_params=pltpu.CompilerParams(collective_id=0, has_side_effects=True, vmem_limit_bytes=49 << 20),
    )(step_count, *[
        pltpu.with_memory_space_constraint(x, pltpu.MemorySpace.HBM)
        for x in (tensor_rows, decay_mask, master, moment_first, moment_second, gradients)
    ])
    return pl.pallas_call(
        store_kernel,
        name="store",
        out_shape=[jax.ShapeDtypeStruct(block, f32)] * 3 + [jax.ShapeDtypeStruct((DP * ROWS, COLS), jnp.bfloat16)],
        in_specs=[vmem] * 4,
        out_specs=[hbm] * 4,
        scratch_shapes=[pltpu.SemaphoreType.DMA((11,))],
        compiler_params=pltpu.CompilerParams(vmem_limit_bytes=4 << 20),
    )(*results)


def solution(mesh):
    placed = (P("dp", "mp"), P("dp", "mp"), P("dp", "mp"), P("dp", "mp"), P(), P(), P())
    return jax.shard_map(
        local,
        mesh=mesh,
        in_specs=placed,
        out_specs=(P("dp", "mp"), P("dp", "mp"), P("dp", "mp"), P(None, "mp")),
        check_vma=False,
    )
```

```python
import functools

import jax
import jax.numpy as jnp
from jax import lax
from jax.experimental import pallas as pl
from jax.experimental.pallas import tpu as pltpu
from jax.sharding import PartitionSpec as P

MESH = pl.DeviceIdType.MESH

beta_first = 0.9
beta_second = 0.999
adam_epsilon = 1e-06
decay_rate = 0.3
learn_rate = 0.3
norm_epsilon = 1e-06

TENSORS = 24
ROWS = 512
COLS = 640
DP = 16
MP = 8
REACH = 3
PEERS = (2 * REACH + 1) * MP

LOAD = 64
LOADS = ROWS // LOAD
PIECE = 32
CHUNKS = (96, 96, 96, 112, 112)
STARTS = tuple(sum(CHUNKS[:k]) for k in range(len(CHUNKS)))
A = (0, 1, 2)
B = (3, 4)
UP = frozenset((0, 2, 3))
UP_CROSSED = frozenset((1,))


def forwards(kind, k):
    if kind == "up1":
        return (("up", "z2"),) * (k in UP) + (("x", "x_up"),) * (k in B)
    if kind == "down1":
        return (("down", "z2"),) * (k not in UP) + (("x", "x_down"),) * (k in B)
    if kind == "z2":
        return (("x", "x_z2"),) * (k in B)
    if kind == "x0":
        return (("up", "x_up"), ("down", "x_down")) if k in A else ()
    if kind == "x_up" and k in A:
        return (("up", "x_z2"),) * (k in UP_CROSSED)
    if kind == "x_down" and k in A:
        return (("down", "x_z2"),) * (k not in UP_CROSSED)
    return ()


def own_order():
    first = [(A[0], "x"), (B[0], "up"), (B[0], "down"), (A[1], "x"), (B[1], "up"), (B[1], "down"), (A[2], "x")]
    return first, [(k, link) for k in A for link in ("up", "down")] + [(k, "x") for k in B]


def arrival_order():
    first = {"up": "up1", "down": "down1", "x": "x0"}
    free = {"up": 0.0, "down": 0.0, "x": 0.0}
    pending, order = [], []

    def send(link, kind, k, now):
        free[link] = max(free[link], now) + CHUNKS[k] / 36.4
        pending.append((free[link] + 2.0, len(pending) + len(order), kind, k))

    for k, link in sum(own_order(), []):
        send(link, first[link], k, 0.0)
    while pending:
        pending.sort()
        now, _, kind, k = pending.pop(0)
        order.append((kind, k))
        for link, there in forwards(kind, k):
            send(link, there, k, now)
    return order


ORDER = arrival_order()
SLOT = {item: n for n, item in enumerate(ORDER)}


def kernel(steps_ref, rows_hbm, decay_hbm, master_hbm, first_hbm, second_hbm, grad_hbm,
           master_out, first_out, second_out, weights,
           master, first, second, grad, update, part, parts, rows_ref, decay_ref, small_sem,
           load_sem, part_send, part_recv, up_send, down_send, x_send, core_send, recv_sem, core_recv):
    d, m = lax.axis_index("dp"), lax.axis_index("mp")
    z, x, c = d // 4, (d // 2) % 2, d % 2
    step = 1 + 2 * c
    z_up, z_down, z_far = (z + step) % 4, (z + 4 - step) % 4, (z + 2) % 4

    def device(zz, xx, cc):
        return (zz * 2 + xx) * 2 + cc

    target = {"up": device(z_up, x, c), "down": device(z_down, x, c), "x": device(z, 1 - x, c)}
    partner = device(z, x, 1 - c)
    send_sem = {"up": up_send, "down": down_send, "x": x_send}

    reaches = sorted(range(-REACH, REACH + 1), key=lambda r: -abs(r))
    others = sorted(((hi, y) for hi in range(2) for y in range(4)), key=lambda p: -(2 * p[0] + min(p[1], 4 - p[1])))

    def inside(reach):
        return (d + reach >= 0) & (d + reach < DP)

    def peers(reach):
        return [
            (d + reach, (m // 4 + hi) % 2 * 4 + (m + y) % 4) for hi, y in others if (reach, hi, y) != (0, 0, 0)
        ]

    def from_reach(reach):
        return parts.at[pl.ds((reach + REACH) * MP, MP - (reach == 0))]

    smalls = [
        pltpu.make_async_copy(src, dst, small_sem.at[n])
        for n, (src, dst) in enumerate(((rows_hbm, rows_ref), (decay_hbm, decay_ref)))
    ]
    for one in smalls:
        one.start()
    for n in range(LOADS):
        span = pl.ds(n * LOAD, LOAD)
        for src, dst in ((master_hbm, master), (first_hbm, first), (second_hbm, second), (grad_hbm, grad)):
            pltpu.make_async_copy(src.at[span], dst.at[span], load_sem.at[n]).start()

    parts[...] = jnp.zeros((PEERS, 1, 128), jnp.float32)
    barrier = pltpu.get_barrier_semaphore()
    for reach in reaches:
        @pl.when(inside(reach))
        def _():
            for pd, pm in peers(reach):
                pl.semaphore_signal(barrier, inc=1, device_id=(pd, pm), device_id_type=MESH)
    for link in ("up", "down"):
        pl.semaphore_signal(barrier, inc=1, device_id=(target[link], m), device_id_type=MESH)

    steps = jnp.full((8, 128), steps_ref[0], jnp.int32)
    power_first = jnp.ones((8, 128), jnp.float32)
    power_second = jnp.ones((8, 128), jnp.float32)
    base_first, base_second = jnp.float32(beta_first), jnp.float32(beta_second)
    base_first = jnp.full((8, 128), base_first)
    base_second = jnp.full((8, 128), base_second)
    for _ in range(31):
        odd = steps % 2 == 1
        power_first = jnp.where(odd, power_first * base_first, power_first)
        power_second = jnp.where(odd, power_second * base_second, power_second)
        base_first, base_second, steps = base_first * base_first, base_second * base_second, steps // 2
    fix_first = 1.0 - power_first
    den_scale = (fix_first * jnp.sqrt(1.0 / (1.0 - power_second)))[:1, :1]
    den_shift = (fix_first * adam_epsilon)[:1, :1]

    lane = lax.broadcasted_iota(jnp.int32, (8, 128), 1)
    sub = lax.broadcasted_iota(jnp.int32, (8, 128), 0)
    for one in smalls:
        one.wait()
    start = jnp.zeros((8, 128), jnp.int32)
    end = jnp.zeros((8, 128), jnp.int32)
    decay = jnp.zeros((8, 128), jnp.float32)
    offset = jnp.int32(0)
    for t in range(TENSORS):
        here = lane % 32 == t
        after = offset + rows_ref[t]
        start = jnp.where(here, offset, start)
        end = jnp.where(here, after, end)
        decay = jnp.where(here, decay_ref[t].astype(jnp.float32) * decay_rate, decay)
        offset = after
    decay = jnp.where(lane < 32, decay, 0.0)

    first_row = d * ROWS

    def member(row):
        ids = sub + (first_row + row)
        return (ids >= start) & (ids < end)

    def load_step(n, total):
        four = master.at[pl.ds(0, 4 * LOAD)]
        pltpu.make_async_copy(four, four, load_sem.at[n]).wait()
        for g in range(LOAD // 8):
            row = n * LOAD + g * 8
            here = pl.ds(pl.multiple_of(row, 8), 8)
            w, gr = master[here, :], grad[here, :]
            new_first = beta_first * first[here, :] + (1.0 - beta_first) * gr
            new_second = beta_second * second[here, :] + (1.0 - beta_second) * gr * gr
            first_out[here, :] = new_first
            second_out[here, :] = new_second
            owned = member(row)
            decay_row = jnp.sum(jnp.where(owned, decay, 0.0), axis=1, keepdims=True)
            up = new_first / (jnp.sqrt(new_second) * den_scale + den_shift) + decay_row * w
            update[here, :] = up
            w_sum = jnp.sum(w * w, axis=1, keepdims=True)
            u_sum = jnp.sum(up * up, axis=1, keepdims=True)
            total = total + jnp.where(owned, jnp.where(lane < 32, w_sum, u_sum), 0.0)
        return total

    total = lax.fori_loop(0, LOADS, load_step, jnp.zeros((8, 128), jnp.float32))
    total = jnp.sum(total, axis=0, keepdims=True)
    part[...] = total
    parts[REACH * MP + m] = total

    blocks = sum(inside(reach).astype(jnp.int32) for reach in reaches)
    pl.semaphore_wait(barrier, blocks * MP + 1)

    for reach in reaches:
        @pl.when(inside(reach))
        def _():
            for pd, pm in peers(reach):
                pltpu.make_async_remote_copy(
                    src_ref=part, dst_ref=parts.at[(REACH - reach) * MP + m],
                    send_sem=part_send.at[REACH - reach], recv_sem=part_recv.at[REACH - reach],
                    device_id=(pd, pm), device_id_type=MESH,
                ).start()

    def drain(sem):
        for reach in reaches:
            @pl.when(inside(reach))
            def _():
                pltpu.make_async_copy(from_reach(reach), from_reach(reach), sem(reach)).wait()

    drain(lambda reach: part_recv.at[REACH + reach])

    sums = jnp.sum(parts[...], axis=0)
    sums = jnp.broadcast_to(sums, (8, 128))
    u_sq = pltpu.roll(sums, 96, 1)
    ratio = learn_rate * (jnp.sqrt(sums) / (jnp.sqrt(u_sq) + norm_epsilon))
    ratio = jnp.where(lane < TENSORS, ratio, 0.0)

    def copy(link, kind, dev, k, part_of=None):
        row, rows = part_of or (STARTS[k], CHUNKS[k])
        span = weights.at[pl.ds(pl.multiple_of(dev * ROWS + row, 16), rows)]
        return pltpu.make_async_remote_copy(
            src_ref=span, dst_ref=span, send_sem=send_sem[link], recv_sem=recv_sem.at[SLOT[kind, k]],
            device_id=(target[link], m), device_id_type=MESH,
        )

    def share(dev, row, rows):
        span = weights.at[pl.ds(pl.multiple_of(dev * ROWS + row, 16), rows)]
        pltpu.make_async_remote_copy(
            src_ref=span, dst_ref=span, send_sem=core_send, recv_sem=core_recv,
            device_id=(partner, m), device_id_type=MESH,
        ).start()

    def finish(first_of, rows):
        for row in range(first_of, first_of + rows, 16):
            halves = []
            for h in (row, row + 8):
                scale = jnp.sum(jnp.where(member(h), ratio, 0.0), axis=1, keepdims=True)
                halves.append(master[pl.ds(h, 8), :] - scale * update[pl.ds(h, 8), :])
            value = jnp.concatenate(halves, axis=0)
            master_out[pl.ds(row, 16), :] = value
            weights[pl.ds(pl.multiple_of(d * ROWS + row, 16), 16), :] = value.astype(jnp.bfloat16)

    first_kind = {"up": "up1", "down": "down1", "x": "x0"}
    pieces = {
        group: [
            (k, STARTS[k] + at, min(PIECE, CHUNKS[k] - at)) for k in group for at in range(0, CHUNKS[k], PIECE)
        ]
        for group in (A, B)
    }
    for turn in range(len(pieces[A])):
        for group, links in ((A, ("x",)), (B, ("up", "down"))):
            if turn < len(pieces[group]):
                k, row, rows = pieces[group][turn]
                finish(row, rows)
                for link in links:
                    copy(link, first_kind[link], d, k, (row, rows)).start()
                share(d, row, rows)
    for k, link in own_order()[1]:
        copy(link, first_kind[link], d, k).start()

    origin = {
        "up1": device(z_down, x, c), "down1": device(z_up, x, c), "z2": device(z_far, x, c),
        "x0": device(z, 1 - x, c), "x_up": device(z_down, 1 - x, c), "x_down": device(z_up, 1 - x, c),
        "x_z2": device(z_far, 1 - x, c),
    }
    sent = {"up": ROWS, "down": ROWS, "x": ROWS}
    for kind, k in ORDER:
        dev = origin[kind]
        copy("x", kind, dev, k).wait_recv()
        for link, there in forwards(kind, k):
            copy(link, there, dev, k).start()
            sent[link] += CHUNKS[k]
        share(dev, STARTS[k], CHUNKS[k])

    def rows_of(count):
        return weights.at[pl.ds(0, count)]

    pltpu.make_async_copy(rows_of(8 * ROWS), rows_of(8 * ROWS), core_recv).wait()
    pltpu.make_async_copy(rows_of(8 * ROWS), rows_of(8 * ROWS), core_send).wait()
    for link, count in sent.items():
        pltpu.make_async_copy(rows_of(count), rows_of(count), send_sem[link]).wait()
    drain(lambda reach: part_send.at[REACH - reach])


def store_kernel(*refs):
    sources, sinks, sem = refs[:4], refs[4:8], refs[8]
    copies = []
    for n, (src, dst) in enumerate(zip(sources, sinks)):
        pieces = 8 if n == 3 else 1
        rows = src.shape[0] // pieces
        for i in range(pieces):
            span = pl.ds(i * rows, rows)
            copies.append(pltpu.make_async_copy(src.at[span], dst.at[span], sem.at[len(copies)]))
    for one in copies:
        one.start()
    for one in copies:
        one.wait()


def local(master, moment_first, moment_second, gradients, step_count, tensor_rows, decay_mask):
    hbm = pl.BlockSpec(memory_space=pltpu.MemorySpace.HBM)
    vmem = pl.BlockSpec(memory_space=pltpu.MemorySpace.VMEM)
    smem = pl.BlockSpec(memory_space=pltpu.MemorySpace.SMEM)
    f32 = jnp.float32
    block = (ROWS, COLS)
    results = pl.pallas_call(
        kernel,
        name="lamb_gather",
        out_shape=[pltpu.VMEM(block, f32)] * 3 + [pltpu.VMEM((DP * ROWS, COLS), jnp.bfloat16)],
        in_specs=[smem] + [hbm] * 6,
        out_specs=[vmem] * 4,
        scratch_shapes=[pltpu.VMEM(block, f32)] * 5 + [
            pltpu.VMEM((1, 128), f32),
            pltpu.VMEM((PEERS, 1, 128), f32),
            pltpu.SMEM((TENSORS,), jnp.int32),
            pltpu.SMEM((TENSORS,), jnp.int32),
            pltpu.SemaphoreType.DMA((2,)),
            pltpu.SemaphoreType.DMA((LOADS,)),
            pltpu.SemaphoreType.DMA((2 * REACH + 1,)),
            pltpu.SemaphoreType.DMA((2 * REACH + 1,)),
        ] + [pltpu.SemaphoreType.DMA] * 4 + [
            pltpu.SemaphoreType.DMA((len(ORDER),)),
            pltpu.SemaphoreType.DMA,
        ],
        compiler_params=pltpu.CompilerParams(collective_id=0, has_side_effects=True, vmem_limit_bytes=49 << 20),
    )(step_count, *[
        pltpu.with_memory_space_constraint(x, pltpu.MemorySpace.HBM)
        for x in (tensor_rows, decay_mask, master, moment_first, moment_second, gradients)
    ])
    return pl.pallas_call(
        store_kernel,
        name="store",
        out_shape=[jax.ShapeDtypeStruct(block, f32)] * 3 + [jax.ShapeDtypeStruct((DP * ROWS, COLS), jnp.bfloat16)],
        in_specs=[vmem] * 4,
        out_specs=[hbm] * 4,
        scratch_shapes=[pltpu.SemaphoreType.DMA((11,))],
        compiler_params=pltpu.CompilerParams(vmem_limit_bytes=4 << 20),
    )(*results)


def solution(mesh):
    placed = (P("dp", "mp"), P("dp", "mp"), P("dp", "mp"), P("dp", "mp"), P(), P(), P())
    return jax.shard_map(
        local,
        mesh=mesh,
        in_specs=placed,
        out_specs=(P("dp", "mp"), P("dp", "mp"), P("dp", "mp"), P(None, "mp")),
        check_vma=False,
    )
```

```python
import functools

import jax
import jax.numpy as jnp
from jax import lax
from jax.experimental import pallas as pl
from jax.experimental.pallas import tpu as pltpu
from jax.sharding import PartitionSpec as P

MESH = pl.DeviceIdType.MESH

beta_first = 0.9
beta_second = 0.999
adam_epsilon = 1e-06
decay_rate = 0.3
learn_rate = 0.3
norm_epsilon = 1e-06

TENSORS = 24
ROWS = 512
COLS = 640
DP = 16
MP = 8
REACH = 3
PEERS = (2 * REACH + 1) * MP

LOAD = 64
LOADS = ROWS // LOAD
PIECE = 32
CHUNKS = (96, 80, 96, 128, 112)
STARTS = tuple(sum(CHUNKS[:k]) for k in range(len(CHUNKS)))
A = (0, 1, 2)
B = (3, 4)
UP = frozenset((0, 1, 4))
UP_CROSSED = frozenset((1,))


def forwards(kind, k):
    if kind == "up1":
        return (("up", "z2"),) * (k in UP) + (("x", "x_up"),) * (k in B)
    if kind == "down1":
        return (("down", "z2"),) * (k not in UP) + (("x", "x_down"),) * (k in B)
    if kind == "z2":
        return (("x", "x_z2"),) * (k in B)
    if kind == "x0":
        return (("up", "x_up"), ("down", "x_down")) if k in A else ()
    if kind == "x_up" and k in A:
        return (("up", "x_z2"),) * (k in UP_CROSSED)
    if kind == "x_down" and k in A:
        return (("down", "x_z2"),) * (k not in UP_CROSSED)
    return ()


def own_order():
    first = [(A[0], "x"), (B[0], "up"), (B[0], "down"), (A[1], "x"), (B[1], "up"), (B[1], "down"), (A[2], "x")]
    return first, [(k, link) for k in A for link in ("up", "down")] + [(k, "x") for k in B]


def arrival_order():
    first = {"up": "up1", "down": "down1", "x": "x0"}
    free = {"up": 0.0, "down": 0.0, "x": 0.0}
    pending, order = [], []

    def send(link, kind, k, now):
        free[link] = max(free[link], now) + CHUNKS[k] / 36.4
        pending.append((free[link] + 2.0, len(pending) + len(order), kind, k))

    for k, link in sum(own_order(), []):
        send(link, first[link], k, 0.0)
    while pending:
        pending.sort()
        now, _, kind, k = pending.pop(0)
        order.append((kind, k))
        for link, there in forwards(kind, k):
            send(link, there, k, now)
    return order


ORDER = arrival_order()
SLOT = {item: n for n, item in enumerate(ORDER)}


def kernel(steps_ref, rows_hbm, decay_hbm, master_hbm, first_hbm, second_hbm, grad_hbm,
           master_out, first_out, second_out, weights,
           master, first, second, grad, update, part, parts, rows_ref, decay_ref, small_sem,
           load_sem, part_send, part_recv, up_send, down_send, x_send, core_send, recv_sem, core_recv):
    d, m = lax.axis_index("dp"), lax.axis_index("mp")
    z, x, c = d // 4, (d // 2) % 2, d % 2
    z_up, z_down, z_far = (z + 1) % 4, (z + 3) % 4, (z + 2) % 4

    def device(zz, xx, cc):
        return (zz * 2 + xx) * 2 + cc

    target = {"up": device(z_up, x, c), "down": device(z_down, x, c), "x": device(z, 1 - x, c)}
    partner = device(z, x, 1 - c)
    send_sem = {"up": up_send, "down": down_send, "x": x_send}

    columns = sorted(((hi, y) for hi in range(2) for y in range(4)), key=lambda p: -(2 * p[0] + min(p[1], 4 - p[1])))

    def inside(reach):
        return (d + reach >= 0) & (d + reach < DP)

    def for_peers(act):
        for reach in (3, -3, 2, -2, 1, -1, 0):
            @pl.when(inside(reach))
            def _():
                for hi, y in columns:
                    if (reach, hi, y) != (0, 0, 0):
                        act(reach, (d + reach, (m // 4 + hi) % 2 * 4 + (m + y) % 4))

    def from_reach(reach):
        return parts.at[pl.ds((reach + REACH) * MP, MP - (reach == 0))]

    smalls = [
        pltpu.make_async_copy(src, dst, small_sem.at[n])
        for n, (src, dst) in enumerate(((rows_hbm, rows_ref), (decay_hbm, decay_ref)))
    ]
    for one in smalls:
        one.start()
    for n in range(LOADS):
        span = pl.ds(n * LOAD, LOAD)
        for src, dst in ((master_hbm, master), (first_hbm, first), (second_hbm, second), (grad_hbm, grad)):
            pltpu.make_async_copy(src.at[span], dst.at[span], load_sem.at[n]).start()

    parts[...] = jnp.zeros((PEERS, 1, 128), jnp.float32)
    barrier = pltpu.get_barrier_semaphore()
    for_peers(lambda reach, peer: pl.semaphore_signal(barrier, inc=1, device_id=peer, device_id_type=MESH))
    for link in ("up", "down"):
        pl.semaphore_signal(barrier, inc=1, device_id=(target[link], m), device_id_type=MESH)

    steps = jnp.full((8, 128), steps_ref[0], jnp.int32)
    power_first = jnp.ones((8, 128), jnp.float32)
    power_second = jnp.ones((8, 128), jnp.float32)
    base_first, base_second = jnp.float32(beta_first), jnp.float32(beta_second)
    base_first = jnp.full((8, 128), base_first)
    base_second = jnp.full((8, 128), base_second)
    for _ in range(31):
        odd = steps % 2 == 1
        power_first = jnp.where(odd, power_first * base_first, power_first)
        power_second = jnp.where(odd, power_second * base_second, power_second)
        base_first, base_second, steps = base_first * base_first, base_second * base_second, steps // 2
    fix_first = 1.0 - power_first
    den_scale = (fix_first * jnp.sqrt(1.0 / (1.0 - power_second)))[:1, :1]
    den_shift = (fix_first * adam_epsilon)[:1, :1]

    lane = lax.broadcasted_iota(jnp.int32, (8, 128), 1)
    sub = lax.broadcasted_iota(jnp.int32, (8, 128), 0)
    for one in smalls:
        one.wait()
    start = jnp.zeros((8, 128), jnp.int32)
    end = jnp.zeros((8, 128), jnp.int32)
    decay = jnp.zeros((8, 128), jnp.float32)
    offset = jnp.int32(0)
    for t in range(TENSORS):
        here = lane % 32 == t
        after = offset + rows_ref[t]
        start = jnp.where(here, offset, start)
        end = jnp.where(here, after, end)
        decay = jnp.where(here, decay_ref[t].astype(jnp.float32) * decay_rate, decay)
        offset = after
    decay = jnp.where(lane < 32, decay, 0.0)

    first_row = d * ROWS

    def member(row):
        ids = sub + (first_row + row)
        return (ids >= start) & (ids < end)

    def load_step(n, total):
        four = master.at[pl.ds(0, 4 * LOAD)]
        pltpu.make_async_copy(four, four, load_sem.at[n]).wait()
        for g in range(LOAD // 8):
            row = n * LOAD + g * 8
            here = pl.ds(pl.multiple_of(row, 8), 8)
            w, gr = master[here, :], grad[here, :]
            new_first = beta_first * first[here, :] + (1.0 - beta_first) * gr
            new_second = beta_second * second[here, :] + (1.0 - beta_second) * gr * gr
            first_out[here, :] = new_first
            second_out[here, :] = new_second
            owned = member(row)
            decay_row = jnp.sum(jnp.where(owned, decay, 0.0), axis=1, keepdims=True)
            root = new_second * lax.rsqrt(new_second)
            up = new_first / (root * den_scale + den_shift) + decay_row * w
            update[here, :] = up
            w_sum = jnp.sum(w * w, axis=1, keepdims=True)
            u_sum = jnp.sum(up * up, axis=1, keepdims=True)
            total = total + jnp.where(owned, jnp.where(lane < 32, w_sum, u_sum), 0.0)
        return total

    total = lax.fori_loop(0, LOADS, load_step, jnp.zeros((8, 128), jnp.float32))
    total = jnp.sum(total, axis=0, keepdims=True)
    part[...] = total
    parts[REACH * MP + m] = total

    blocks = sum(inside(reach).astype(jnp.int32) for reach in range(-REACH, REACH + 1))
    pl.semaphore_wait(barrier, blocks * MP + 1)

    for_peers(lambda reach, peer: pltpu.make_async_remote_copy(
        src_ref=part, dst_ref=parts.at[(REACH - reach) * MP + m],
        send_sem=part_send.at[REACH - reach], recv_sem=part_recv.at[REACH - reach],
        device_id=peer, device_id_type=MESH,
    ).start())

    def drain(sem):
        for reach in range(-REACH, REACH + 1):
            @pl.when(inside(reach))
            def _():
                pltpu.make_async_copy(from_reach(reach), from_reach(reach), sem(reach)).wait()

    drain(lambda reach: part_recv.at[REACH + reach])

    sums = jnp.sum(parts[...], axis=0)
    sums = jnp.broadcast_to(sums, (8, 128))
    u_sq = pltpu.roll(sums, 96, 1)
    ratio = learn_rate * (jnp.sqrt(sums) / (jnp.sqrt(u_sq) + norm_epsilon))
    ratio = jnp.where(lane < TENSORS, ratio, 0.0)

    def copy(link, kind, dev, k, part_of=None):
        row, rows = part_of or (STARTS[k], CHUNKS[k])
        span = weights.at[pl.ds(pl.multiple_of(dev * ROWS + row, 16), rows)]
        return pltpu.make_async_remote_copy(
            src_ref=span, dst_ref=span, send_sem=send_sem[link], recv_sem=recv_sem.at[SLOT[kind, k]],
            device_id=(target[link], m), device_id_type=MESH,
        )

    def share(dev, row, rows):
        span = weights.at[pl.ds(pl.multiple_of(dev * ROWS + row, 16), rows)]
        pltpu.make_async_remote_copy(
            src_ref=span, dst_ref=span, send_sem=core_send, recv_sem=core_recv,
            device_id=(partner, m), device_id_type=MESH,
        ).start()

    def finish(first_of, rows):
        for row in range(first_of, first_of + rows, 16):
            halves = []
            for h in (row, row + 8):
                scale = jnp.sum(jnp.where(member(h), ratio, 0.0), axis=1, keepdims=True)
                halves.append(master[pl.ds(h, 8), :] - scale * update[pl.ds(h, 8), :])
            value = jnp.concatenate(halves, axis=0)
            master_out[pl.ds(row, 16), :] = value
            weights[pl.ds(pl.multiple_of(d * ROWS + row, 16), 16), :] = value.astype(jnp.bfloat16)

    first_kind = {"up": "up1", "down": "down1", "x": "x0"}
    pieces = {
        group: [
            (k, STARTS[k] + at, min(PIECE, CHUNKS[k] - at)) for k in group for at in range(0, CHUNKS[k], PIECE)
        ]
        for group in (A, B)
    }
    for turn in range(len(pieces[A])):
        for group, links in ((A, ("x",)), (B, ("up", "down"))):
            if turn < len(pieces[group]):
                k, row, rows = pieces[group][turn]
                finish(row, rows)
                for link in links:
                    copy(link, first_kind[link], d, k, (row, rows)).start()
                share(d, row, rows)
    for k, link in own_order()[1]:
        copy(link, first_kind[link], d, k).start()

    origin = {
        "up1": device(z_down, x, c), "down1": device(z_up, x, c), "z2": device(z_far, x, c),
        "x0": device(z, 1 - x, c), "x_up": device(z_down, 1 - x, c), "x_down": device(z_up, 1 - x, c),
        "x_z2": device(z_far, 1 - x, c),
    }
    sent = {"up": ROWS, "down": ROWS, "x": ROWS}
    for kind, k in ORDER:
        dev = origin[kind]
        copy("x", kind, dev, k).wait_recv()
        for link, there in forwards(kind, k):
            copy(link, there, dev, k).start()
            sent[link] += CHUNKS[k]
        share(dev, STARTS[k], CHUNKS[k])

    def rows_of(count):
        return weights.at[pl.ds(0, count)]

    pltpu.make_async_copy(rows_of(8 * ROWS), rows_of(8 * ROWS), core_recv).wait()
    pltpu.make_async_copy(rows_of(8 * ROWS), rows_of(8 * ROWS), core_send).wait()
    for link, count in sent.items():
        pltpu.make_async_copy(rows_of(count), rows_of(count), send_sem[link]).wait()
    drain(lambda reach: part_send.at[REACH - reach])


def store_kernel(*refs):
    sources, sinks, sem = refs[:4], refs[4:8], refs[8]
    copies = []
    for n, (src, dst) in enumerate(zip(sources, sinks)):
        pieces = 8 if n == 3 else 1
        rows = src.shape[0] // pieces
        for i in range(pieces):
            span = pl.ds(i * rows, rows)
            copies.append(pltpu.make_async_copy(src.at[span], dst.at[span], sem.at[len(copies)]))
    for one in copies:
        one.start()
    for one in copies:
        one.wait()


def local(master, moment_first, moment_second, gradients, step_count, tensor_rows, decay_mask):
    hbm = pl.BlockSpec(memory_space=pltpu.MemorySpace.HBM)
    vmem = pl.BlockSpec(memory_space=pltpu.MemorySpace.VMEM)
    smem = pl.BlockSpec(memory_space=pltpu.MemorySpace.SMEM)
    f32 = jnp.float32
    block = (ROWS, COLS)
    results = pl.pallas_call(
        kernel,
        name="lamb_gather",
        out_shape=[pltpu.VMEM(block, f32)] * 3 + [pltpu.VMEM((DP * ROWS, COLS), jnp.bfloat16)],
        in_specs=[smem] + [hbm] * 6,
        out_specs=[vmem] * 4,
        scratch_shapes=[pltpu.VMEM(block, f32)] * 5 + [
            pltpu.VMEM((1, 128), f32),
            pltpu.VMEM((PEERS, 1, 128), f32),
            pltpu.SMEM((TENSORS,), jnp.int32),
            pltpu.SMEM((TENSORS,), jnp.int32),
            pltpu.SemaphoreType.DMA((2,)),
            pltpu.SemaphoreType.DMA((LOADS,)),
            pltpu.SemaphoreType.DMA((2 * REACH + 1,)),
            pltpu.SemaphoreType.DMA((2 * REACH + 1,)),
        ] + [pltpu.SemaphoreType.DMA] * 4 + [
            pltpu.SemaphoreType.DMA((len(ORDER),)),
            pltpu.SemaphoreType.DMA,
        ],
        compiler_params=pltpu.CompilerParams(collective_id=0, has_side_effects=True, vmem_limit_bytes=49 << 20),
    )(step_count, *[
        pltpu.with_memory_space_constraint(x, pltpu.MemorySpace.HBM)
        for x in (tensor_rows, decay_mask, master, moment_first, moment_second, gradients)
    ])
    return pl.pallas_call(
        store_kernel,
        name="store",
        out_shape=[jax.ShapeDtypeStruct(block, f32)] * 3 + [jax.ShapeDtypeStruct((DP * ROWS, COLS), jnp.bfloat16)],
        in_specs=[vmem] * 4,
        out_specs=[hbm] * 4,
        scratch_shapes=[pltpu.SemaphoreType.DMA((11,))],
        compiler_params=pltpu.CompilerParams(vmem_limit_bytes=4 << 20),
    )(*results)


def solution(mesh):
    placed = (P("dp", "mp"), P("dp", "mp"), P("dp", "mp"), P("dp", "mp"), P(), P(), P())
    return jax.shard_map(
        local,
        mesh=mesh,
        in_specs=placed,
        out_specs=(P("dp", "mp"), P("dp", "mp"), P("dp", "mp"), P(None, "mp")),
        check_vma=False,
    )
```
